128 devices in a mesh: expert: 64 (over y, x, z), etp: 2 (over core).
Axes of the slice: x: 4, y: 4, z: 4, core: 2. Of those that a mesh axis runs over, the one named last changes fastest.
Arguments:
- grad_out: bfloat16 [8192, 3584], P('expert', 'etp'), may hold values from -6 to 6
- combine: bfloat16 [8192, 8], P('expert'), may hold values from 0.099609375 to 2.5
- expert_ids: int32 [8192, 8], P('expert'), may hold values from 0 to 127, all different within a row; in each aligned block of 128 rows (0 to 127, 128 to 255, ...) at most 16 rows name the same one
- saved_gate: bfloat16 [1024, 128, 1024], P(None, 'expert', 'etp'), may hold values from -6 to 6
- saved_up: bfloat16 [1024, 128, 1024], P(None, 'expert', 'etp'), may hold values from -1.5 to 1.5
- gate_weight: bfloat16 [128, 3584, 1024], P('expert', None, 'etp'), may hold values from -0.09375 to 0.09375
- up_weight: bfloat16 [128, 3584, 1024], P('expert', None, 'etp'), may hold values from -0.09375 to 0.09375
- down_weight: bfloat16 [128, 1024, 3584], P('expert', 'etp'), may hold values from -0.09375 to 0.09375
Outputs:
- grad_tokens: bfloat16 [8192, 3584], P('expert', 'etp')
- grad_combine: bfloat16 [8192, 8], P('expert')
The draws below stay inside these ranges and needn't reach their ends.
Inputs may be any that keep to these rules, and one draw needn't show every extreme that they name: `expert_ids`: each token names 8 different experts. Among the 128 tokens of one block (one index of expert), at most 16 name any one expert, and some blocks reach that bound.
All inputs are finite; a program needn't handle non-finite values.
Results may differ from the reference program's by a relative error of at most 0.012.
Values may be sent and summed in bfloat16 or wider, within the bound.
No kernel may reach another device: no remote copies, remote signals or barrier semaphores. Data moves between devices by JAX's collectives and lax.ppermute only.
A program may use at most 192 MiB of HBM per device.

```python
import math
import jax
import jax.numpy as jnp
import numpy as np
from jax import lax

D = 3584
FF = 1024
TOP = 8
TOK_DEV = 128
EXPERTS = 128
TOKENS = 8192
CAP = 16
SLOT_ROWS = 1024
N_EXPERT = 64
N_ETP = 2


def steps_of(stream_key, extent, shards, smallest, top_value):
    gain = 1.0
    for axis_at, parts in shards:
        draws = jax.random.uniform(jax.random.fold_in(jax.random.fold_in(stream_key, 6), axis_at), (parts,), jnp.float32, smallest / len(shards), top_value / len(shards))
        gain = gain * jnp.repeat(jnp.exp(draws), extent[axis_at] // parts).reshape((-1,) + (1,) * (len(extent) - 1 - axis_at))
    return gain


def shared_out(rng, own, number, rows, amount, top, limit, slope):
    sequence = jax.random.permutation(rng, amount)
    crowded, ordinary = portions_of(amount, rows * top, limit, slope, True), portions_of(amount, rows * top, limit, slope, False)
    places = jnp.arange(amount)

    def named(sizes, rotation):
        used = int((sizes > 0).sum())
        fixed = max(1, used // 4)
        passed = fixed + (places - fixed + rotation * (used - fixed)) % max(1, amount - fixed)
        return jnp.zeros((amount,), jnp.int32).at[sequence[jnp.where(places < fixed, places, passed)]].set(jnp.asarray(sizes, jnp.int32))

    sizes = jnp.where(number % 4 == 0, named(crowded, number // 4), named(ordinary, number - number // 4 - 1))
    mixed = jax.random.permutation(jax.random.fold_in(own, 3), amount)
    source_of, taker = mixed[0:amount // 2 * 2:2], mixed[1:amount // 2 * 2:2]
    room = jnp.minimum(sizes[source_of] - 1, limit - sizes[taker]) // 2
    room = jnp.where((source_of == sequence[0]) | (taker == sequence[0]) | (sizes[taker] == 0), 0, jnp.maximum(room, 0))
    passed = jax.random.randint(jax.random.fold_in(own, 4), (amount // 2,), 0, 1 << 20) % (room + 1)
    sizes = sizes.at[source_of].add(-passed).at[taker].add(passed)
    labels = jnp.searchsorted(jnp.cumsum(sizes), jnp.arange(rows * top), side="right").astype(jnp.int32)
    grid = labels.reshape(top, rows).T
    grid = grid[jax.random.permutation(jax.random.fold_in(own, 1), rows)]
    rotation = jax.random.randint(jax.random.fold_in(own, 2), (rows, 1), 0, top)
    return jnp.take_along_axis(grid, (jnp.arange(top)[None, :] + rotation) % top, axis=1)


def portions_of(count, total, bound, slope, full):
    loads = [(1 << 20) // math.isqrt(standing ** slope) + 1 for standing in range(1, count + 1)]
    largest = bound if full else min(bound, max(-(-total // count), total * loads[0] // sum(loads)))
    least = 1 if total - largest >= count - 1 else 0
    given, spare = [largest] + [least] * (count - 1), total - largest - least * (count - 1)
    while spare > 0:
        free = [i for i in range(1, count) if given[i] < largest] or [i for i in range(1, count) if given[i] < bound]
        whole, remaining = sum([loads[i] for i in free]), spare
        for i in free:
            more = min(bound - given[i], max(1, remaining * loads[i] // whole), spare)
            given[i] = given[i] + more
            spare = spare - more
    return np.array(given)


def gaussian(key, extent, spread, most, cuts=(), held_as=jnp.bfloat16):
    level = steps_of(key, extent, cuts, -0.22, 0.18) if cuts else 1.0
    drawn = jax.random.normal(key, extent, jnp.float32) * spread * level
    return jnp.minimum(jnp.maximum(drawn, -most), most).astype(held_as)


def setup_inputs(seed: int = 0) -> dict:
    keys = jax.random.split(jax.random.key(seed), 9)
    grad_out = gaussian(keys[0], (TOKENS, D), 1.0, 6.0, ((0, 64), (1, 2)))
    combine = jnp.clip(jnp.exp(math.log(2.5) - 3.2227897 * jax.random.uniform(keys[1], (TOKENS, TOP), jnp.float32) ** steps_of(keys[1], (TOKENS, TOP), ((0, 64),), -0.2, 0.2)), 0.099609375, 2.5).astype(jnp.bfloat16)
    expert_ids_keys = jax.random.split(jax.random.fold_in(keys[2], 1), TOKENS // TOK_DEV)
    expert_ids_turns = jax.random.permutation(jax.random.fold_in(keys[2], 3), TOKENS // TOK_DEV)
    expert_ids = jax.vmap(lambda own, number: shared_out(jax.random.fold_in(keys[2], 2), own, number, TOK_DEV, EXPERTS, TOP, CAP, 2))(expert_ids_keys, expert_ids_turns).reshape((TOKENS, TOP))
    saved_gate = gaussian(keys[3], (SLOT_ROWS, EXPERTS, FF), 1.0, 6.0, ((1, 64), (2, 2)))
    saved_up = gaussian(keys[4], (SLOT_ROWS, EXPERTS, FF), 0.1, 1.5, ((1, 64), (2, 2)))
    gate_weight = gaussian(keys[5], (EXPERTS, D, FF), D ** -0.5, 0.09375, ((0, 64), (2, 2)))
    up_weight = gaussian(keys[6], (EXPERTS, D, FF), D ** -0.5, 0.09375, ((0, 64), (2, 2)))
    down_weight = gaussian(keys[7], (EXPERTS, FF, D), D ** -0.5, 0.09375, ((0, 64), (1, 2)))
    return dict(grad_out=grad_out, combine=combine, expert_ids=expert_ids, saved_gate=saved_gate, saved_up=saved_up, gate_weight=gate_weight, up_weight=up_weight, down_weight=down_weight)


def reference(grad_out, combine, expert_ids, saved_gate, saved_up, gate_weight, up_weight, down_weight):
    token_total, top_count = expert_ids.shape
    experts, model_width, hidden = gate_weight.shape
    groups = N_EXPERT
    token_count = token_total // groups
    capacity = saved_gate.shape[0] // groups
    slot_total = groups * capacity
    grouped = expert_ids.reshape(groups, token_count, top_count)
    matches = grouped[..., None] == jnp.arange(experts, dtype=jnp.int32)
    expert_loads = jnp.sum(matches.astype(jnp.int32), axis=2)
    earlier = jnp.cumsum(expert_loads, axis=1) - expert_loads
    position = jnp.sum(jnp.where(matches, earlier[:, :, None, :], 0), axis=3)
    row_index = (jnp.arange(groups, dtype=jnp.int32)[:, None, None] * capacity + position).reshape(token_total, top_count)
    slot_owner = jnp.full((slot_total, experts), token_total * top_count, jnp.int32)
    slot_owner = slot_owner.at[row_index.reshape(-1), expert_ids.reshape(-1)].set(
        jnp.arange(token_total * top_count, dtype=jnp.int32))
    grad_padded = jnp.concatenate([grad_out, jnp.zeros((1, model_width), jnp.bfloat16)], axis=0)
    weight_padded = jnp.concatenate([combine.reshape(-1).astype(jnp.float32), jnp.zeros((1,), jnp.float32)])
    half_hidden = hidden // N_ETP

    def per_expert(running, expert):
        grad_acc, weight_acc = running
        slot_ids = lax.dynamic_index_in_dim(slot_owner, expert, 1, keepdims=False)
        token_of = slot_ids // top_count
        slot_rows = jnp.take(grad_padded, token_of, axis=0)
        slot_weight = jnp.take(weight_padded, slot_ids, axis=0)
        gate_value = lax.dynamic_index_in_dim(saved_gate, expert, 1, keepdims=False).astype(jnp.float32)
        up_value = lax.dynamic_index_in_dim(saved_up, expert, 1, keepdims=False).astype(jnp.float32)
        down_expert = lax.dynamic_index_in_dim(down_weight, expert, 0, keepdims=False)
        gate_expert = lax.dynamic_index_in_dim(gate_weight, expert, 0, keepdims=False)
        up_expert = lax.dynamic_index_in_dim(up_weight, expert, 0, keepdims=False)
        grad_hidden = jnp.dot(slot_rows, down_expert.T, preferred_element_type=jnp.float32)
        gate_sigmoid = jax.nn.sigmoid(gate_value)
        activated = gate_value * gate_sigmoid
        product = grad_hidden * activated * up_value
        weight_halves = jnp.sum(product.reshape(slot_total, N_ETP, half_hidden), axis=2).astype(jnp.bfloat16)
        weight_halves = lax.optimization_barrier(weight_halves).astype(jnp.float32)
        slot_dw = jnp.sum(weight_halves, axis=1).astype(jnp.bfloat16)
        scaled = slot_weight[:, None] * grad_hidden
        grad_gate = (scaled * up_value * gate_sigmoid * (1.0 + gate_value * (1.0 - gate_sigmoid))).astype(jnp.bfloat16)
        grad_up = (scaled * activated).astype(jnp.bfloat16)
        running_sum = jnp.zeros((slot_total, model_width), jnp.float32)
        for half_index in range(N_ETP):
            lower = half_index * half_hidden
            term_half = jnp.dot(grad_gate[:, lower:lower + half_hidden], gate_expert[:, lower:lower + half_hidden].T,
                                preferred_element_type=jnp.float32)
            term_half = term_half + jnp.dot(grad_up[:, lower:lower + half_hidden], up_expert[:, lower:lower + half_hidden].T,
                                            preferred_element_type=jnp.float32)
            term_half = lax.optimization_barrier(term_half.astype(jnp.bfloat16))
            running_sum = running_sum + term_half.astype(jnp.float32)
        slot_grad = running_sum.astype(jnp.bfloat16)
        grad_acc = grad_acc.at[token_of].add(slot_grad.astype(jnp.float32), mode="drop")
        weight_acc = weight_acc.at[slot_ids].set(slot_dw.astype(jnp.float32), mode="drop")
        return (grad_acc, weight_acc), None

    start = (jnp.zeros((token_total, model_width), jnp.float32), jnp.zeros((token_total * top_count,), jnp.float32))
    final, _ = lax.scan(per_expert, start, jnp.arange(experts, dtype=jnp.int32))
    grad_tokens = final[0].astype(jnp.bfloat16)
    grad_combine = final[1].reshape(token_total, top_count).astype(jnp.bfloat16)
    return grad_tokens, grad_combine
```

```python
import functools

import jax
import jax.numpy as jnp
from jax import lax
from jax.experimental import pallas as pl
from jax.experimental.pallas import tpu as pltpu
from jax.sharding import PartitionSpec as P

BOTH = ("expert", "etp")
CHUNKS = 1
F32 = jnp.float32
BF16 = jnp.bfloat16


def places(ids_ref, experts):
    top, tokens = ids_ref.shape
    ids = ids_ref[...]
    names = lax.broadcasted_iota(jnp.int32, (experts, tokens), 0)
    hits = [ids[k:k + 1, :] == names for k in range(top)]
    member = functools.reduce(jnp.logical_or, hits)
    earlier = (
        lax.broadcasted_iota(jnp.int32, (tokens, tokens), 0)
        < lax.broadcasted_iota(jnp.int32, (tokens, tokens), 1)
    )
    before = jnp.dot(
        member.astype(F32).astype(BF16), earlier.astype(F32).astype(BF16),
        preferred_element_type=F32,
    )
    return hits, jnp.where(member, before, -1.0)


def pack_kernel(first, ids_ref, tokens_ref, out_ref, place_ref):
    step = pl.program_id(0)
    batch, depth, _ = out_ref.shape
    experts = place_ref.shape[0]

    @pl.when(step == 0)
    def _():
        place_ref[...] = places(ids_ref, experts)[1]

    place = place_ref[pl.ds(step * batch, batch), :]
    slots = first + lax.broadcasted_iota(jnp.int32, (batch, depth, place.shape[1]), 1)
    pick = (place[:, None, :] == slots.astype(F32)).astype(F32)
    pick = pick.reshape(batch * depth, place.shape[1]).astype(BF16)
    out = jnp.dot(pick, tokens_ref[...], preferred_element_type=F32)
    out_ref[...] = out.astype(BF16).reshape(out_ref.shape)


def pack(ids, tokens, experts, first, depth):
    count, width = tokens.shape
    batch = 256 // depth
    return pl.pallas_call(
        functools.partial(pack_kernel, first),
        grid=(experts // batch,),
        in_specs=[
            pl.BlockSpec(ids.shape, lambda i: (0, 0)),
            pl.BlockSpec(tokens.shape, lambda i: (0, 0)),
        ],
        out_specs=pl.BlockSpec((batch, depth, width), lambda i: (i, 0, 0)),
        out_shape=jax.ShapeDtypeStruct((experts, depth, width), BF16),
        scratch_shapes=[pltpu.VMEM((experts, count), F32)],
        name=f"pack_{first}",
    )(ids, tokens)


def expert_kernel(
    which_ref, arrived_ref, gate_own, gate_other, up_own, up_other,
    down_mine, down_sent, gatew_mine, gatew_sent, upw_mine, upw_sent,
    back_ref, weight_ref, down_v, mix_v, sems,
):
    step = pl.program_id(0)
    half = down_v.shape[0] // 2
    mine = which_ref[0]
    copies = [
        pltpu.make_async_copy(down_mine.at[mine], down_v.at[0:half], sems.at[0]),
        pltpu.make_async_copy(down_sent, down_v.at[half:2 * half], sems.at[1]),
        pltpu.make_async_copy(gatew_mine.at[mine], mix_v.at[:, 0:half], sems.at[2]),
        pltpu.make_async_copy(gatew_sent, mix_v.at[:, half:2 * half], sems.at[3]),
        pltpu.make_async_copy(upw_mine.at[mine], mix_v.at[:, 2 * half:3 * half], sems.at[4]),
        pltpu.make_async_copy(upw_sent, mix_v.at[:, 3 * half:4 * half], sems.at[5]),
    ]

    @pl.when(step == 0)
    def _():
        for copy in copies:
            copy.start()
        copies[0].wait()
        copies[1].wait()

    groups, halves, depth, width = arrived_ref.shape
    rows = groups * depth
    dims = (((1,), (1,)), ((), ()))
    grad = None
    for h in range(halves):
        part = lax.dot_general(
            arrived_ref[:, h].reshape(rows, width),
            down_v[:, h * width:(h + 1) * width], dims, preferred_element_type=F32,
        )
        grad = part if grad is None else grad + part
    mixed = []
    total = None
    for i, (gate_ref, up_ref) in enumerate(((gate_own, up_own), (gate_other, up_other))):
        g = grad[:, i * half:(i + 1) * half]
        gate = gate_ref[...].reshape(rows, half).astype(F32)
        up = up_ref[...].reshape(rows, half).astype(F32)
        s = jax.nn.sigmoid(gate)
        act = gate * s
        g_act = g * act
        product = g_act * up
        mixed.append(((g * up) * (s * (1.0 + gate * (1.0 - s)))).astype(BF16))
        mixed.append(g_act.astype(BF16))
        for j in range(half // 128):
            term = product[:, j * 128:(j + 1) * 128]
            total = term if total is None else total + term
    weight_ref[...] = jnp.sum(total.T, axis=0, keepdims=True).reshape(weight_ref.shape)

    @pl.when(step == 0)
    def _():
        for copy in copies[2:]:
            copy.wait()

    joined = jnp.concatenate([mixed[0], mixed[2], mixed[1], mixed[3]], axis=1)
    for h in range(halves):
        out = lax.dot_general(
            joined, mix_v[h * width:(h + 1) * width, :], dims, preferred_element_type=F32,
        )
        back_ref[:, h] = out.astype(BF16).reshape(groups, depth, width)


def expert_step(mine, arrived, saved, weights, first):
    groups, halves, depth, width = arrived.shape
    half = saved[0].shape[-1]
    batch = 256 // depth
    steps = groups // batch
    part = first // depth

    saved_spec = pl.BlockSpec((batch, depth, half), lambda i, s: (i, part, 0))
    hbm = pl.BlockSpec(memory_space=pl.ANY)
    return pl.pallas_call(
        expert_kernel,
        grid_spec=pltpu.PrefetchScalarGridSpec(
            num_scalar_prefetch=1,
            grid=(steps,),
            in_specs=[
                pl.BlockSpec((batch, halves, depth, width), lambda i, s: (i, 0, 0, 0)),
                saved_spec, saved_spec, saved_spec, saved_spec,
                hbm, hbm, hbm, hbm, hbm, hbm,
            ],
            out_specs=[
                pl.BlockSpec((batch, halves, depth, width), lambda i, s: (i, 0, 0, 0)),
                pl.BlockSpec((1, 1, batch * depth), lambda i, s: (i, 0, 0)),
            ],
            scratch_shapes=[
                pltpu.VMEM((2 * half, halves * width), BF16),
                pltpu.VMEM((halves * width, 4 * half), BF16),
                pltpu.SemaphoreType.DMA((6,)),
            ],
        ),
        out_shape=[
            jax.ShapeDtypeStruct((groups, halves, depth, width), BF16),
            jax.ShapeDtypeStruct((steps, 1, batch * depth), F32),
        ],
        compiler_params=pltpu.CompilerParams(vmem_limit_bytes=58 * 1024 * 1024),
        name=f"expert_{first}",
    )(mine, arrived, *saved, *weights)


def merge_kernel(chunks, ids_ref, combine_ref, *refs):
    back_refs, dw_refs = refs[:chunks], refs[chunks:2 * chunks]
    tokens_ref, grad_combine_ref, place_ref, share_ref, sum_ref = refs[2 * chunks:]
    step = pl.program_id(0)
    batch, depth, width = back_refs[0].shape
    experts, count = place_ref.shape
    top = ids_ref.shape[0]

    @pl.when(step == 0)
    def _():
        hits, place = places(ids_ref, experts)
        place_ref[...] = place
        share = jnp.zeros((experts, count), F32)
        for k in range(top):
            share = share + jnp.where(hits[k], combine_ref[k:k + 1, :].astype(F32), 0.0)
        share_ref[...] = share
        sum_ref[...] = jnp.zeros_like(sum_ref)
        found = jnp.zeros((experts, count), F32)
        for n in range(chunks):
            for c in range(depth):
                value = dw_refs[n][:, c:c + 1].astype(F32)
                found = found + jnp.where(place == float(n * depth + c), value, 0.0)
        rows = [
            jnp.sum(jnp.where(hits[k], found, 0.0), axis=0, keepdims=True) for k in range(top)
        ]
        grad_combine_ref[...] = jnp.concatenate(rows, axis=0).astype(BF16)

    here = pl.ds(step * batch, batch)
    place, share = place_ref[here, :], share_ref[here, :]
    for n in range(chunks):
        slots = n * depth + lax.broadcasted_iota(jnp.int32, (batch, depth, count), 1)
        take = jnp.where(place[:, None, :] == slots.astype(F32), share[:, None, :], 0.0)
        take = take.reshape(batch * depth, count)
        sum_ref[...] += jnp.dot(
            take.T.astype(BF16), back_refs[n][...].reshape(batch * depth, width),
            preferred_element_type=F32,
        )

    @pl.when(step == pl.num_programs(0) - 1)
    def _():
        tokens_ref[...] = sum_ref[...].astype(BF16)


def merge(ids, combine, backs, dws):
    experts, depth, width = backs[0].shape
    top, count = ids.shape
    chunks = len(backs)
    batch = 256 // depth // chunks
    whole = lambda x: pl.BlockSpec(x.shape, lambda i: (0, 0))
    return pl.pallas_call(
        functools.partial(merge_kernel, chunks),
        grid=(experts // batch,),
        in_specs=[whole(ids), whole(combine)]
        + [pl.BlockSpec((batch, depth, width), lambda i: (i, 0, 0))] * chunks
        + [whole(x) for x in dws],
        out_specs=[
            pl.BlockSpec((count, width), lambda i: (0, 0)),
            pl.BlockSpec((top, count), lambda i: (0, 0)),
        ],
        out_shape=[
            jax.ShapeDtypeStruct((count, width), BF16),
            jax.ShapeDtypeStruct((top, count), BF16),
        ],
        scratch_shapes=[
            pltpu.VMEM((experts, count), F32),
            pltpu.VMEM((experts, count), F32),
            pltpu.VMEM((count, width), F32),
        ],
        name="merge",
    )(ids, combine, *backs, *dws)


def on_device(
    grad_out, combine, expert_ids, saved_gate, saved_up, gate_weight, up_weight, down_weight
):
    groups = lax.axis_size("expert")
    halves = lax.axis_size("etp")
    mine = lax.axis_index("etp")
    experts = groups * gate_weight.shape[0]
    width = grad_out.shape[1]
    capacity = saved_gate.shape[0] // groups
    depth = capacity // CHUNKS
    ids, shares = expert_ids.T, combine.T

    swap = [(0, 1), (1, 0)]

    def both(x, axis):
        own = lax.dynamic_index_in_dim(x, mine, axis, keepdims=False)
        other = lax.dynamic_index_in_dim(x, 1 - mine, axis, keepdims=False)
        return own, lax.ppermute(other, "etp", swap)

    arrivals = []
    for n in range(CHUNKS):
        outgoing = pack(ids, grad_out, experts, n * depth, depth)
        arrivals.append(
            lax.all_to_all(outgoing, BOTH, split_axis=0, concat_axis=0, tiled=True)
        )
    weights = []
    for x in (down_weight, gate_weight, up_weight):
        other = lax.dynamic_index_in_dim(x, 1 - mine, 0, keepdims=False)
        weights += [x, lax.ppermute(other, "etp", swap)]
    saved = []
    for x in (saved_gate, saved_up):
        for y in both(x, 1):
            saved.append(y.reshape(groups, capacity, y.shape[-1]))

    returned, returned_dw = [], []
    for n in range(CHUNKS):
        back, dw = expert_step(
            mine.reshape(1), arrivals[n].reshape(groups, halves, depth, width),
            saved, weights, n * depth,
        )
        dw = dw.reshape(groups, 1, depth).astype(BF16)
        dw = jnp.broadcast_to(dw, (groups, halves, depth)).reshape(experts, depth)
        returned_dw.append(lax.all_to_all(dw, BOTH, split_axis=0, concat_axis=0, tiled=True))
        returned.append(
            lax.all_to_all(
                back.reshape(groups * halves, depth, width), BOTH,
                split_axis=0, concat_axis=0, tiled=True,
            )
        )
    grad_tokens, grad_combine = merge(ids, shares, returned, returned_dw)
    return grad_tokens, grad_combine.T


def solution(mesh):
    in_specs = (
        P("expert", "etp"),
        P("expert", None),
        P("expert", None),
        P(None, "expert", "etp"),
        P(None, "expert", "etp"),
        P("expert", None, "etp"),
        P("expert", None, "etp"),
        P("expert", "etp", None),
    )
    out_specs = (P("expert", "etp"), P("expert", None))
    return jax.shard_map(
        on_device, mesh=mesh, in_specs=in_specs, out_specs=out_specs, check_vma=False
    )
```

```python
import functools

import jax
import jax.numpy as jnp
from jax import lax
from jax.experimental import pallas as pl
from jax.experimental.pallas import tpu as pltpu
from jax.sharding import PartitionSpec as P


BOTH = ("expert", "etp")
SIDE = 4
TOP = 8
LANES = 128
META = 16
BATCH = 2
SEND = (2, 1, 3)
F32 = jnp.float32
BF16 = jnp.bfloat16
WIDE = ((0, 1, 2), (1, 2, 0))
NARROW = ((2, 0, 1), (2, 0, 1))
NT = (((1,), (1,)), ((), ()))


def coords(e):
    return [e // (SIDE * SIDE), (e // SIDE) % SIDE, e % SIDE]


def joined(c):
    return (c[0] * SIDE + c[1]) * SIDE + c[2]


def moved(x, lane, stage, distance):
    pairs = []
    for e in range(SIDE ** 3):
        for core in range(2):
            to = coords(e)
            axis = lane[core][stage]
            to[axis] = (to[axis] - distance) % SIDE
            pairs.append((e * 2 + core, joined(to) * 2 + core))
    return lax.ppermute(x, BOTH, pairs)


def gathered(x, lane, stage):
    got = {q: moved(x, lane, stage, q) for q in SEND}
    return [x, got[1], got[2], got[3]]


def scattered(parts, lane, stage):
    got = {q: moved(parts[-q % SIDE], lane, stage, q) for q in SEND}
    return [parts[0], got[1], got[2], got[3]]


def prepare_kernel(tiles, grad_ref, ids_ref, share_ref, *outs):
    first = 0
    for out, count in zip(outs, tiles):
        for i in range(count):
            column = (first + i) * LANES
            out[i * LANES:(i + 1) * LANES, :] = grad_ref[:, column:column + LANES]
        out[count * LANES:count * LANES + TOP, :] = ids_ref[...].astype(F32).astype(BF16)
        out[count * LANES + TOP:count * LANES + META, :] = share_ref[...]
        first += count


def prepare(grad_out, ids, shares, tiles):
    return pl.pallas_call(
        functools.partial(prepare_kernel, tiles),
        out_shape=[jax.ShapeDtypeStruct((n * LANES + META, LANES), BF16) for n in tiles],
        name="prepare",
    )(grad_out, ids, shares)


def settle(names_ref, metas, place_ref, share_ref=None):
    tokens = metas[0].shape[2]
    experts = 2 * SIDE
    at = lax.broadcasted_iota(jnp.int32, (experts, tokens), 0)
    names = jnp.zeros((experts, tokens), jnp.int32)
    for i in range(experts):
        names = jnp.where(at == i, names_ref[i], names)
    names = names.astype(F32)
    members, weights = [], []
    for i in range(SIDE):
        for j in range(SIDE):
            ids = metas[j][i, 0:TOP, :].astype(F32)
            shares = metas[j][i, TOP:META, :].astype(F32)
            member = jnp.zeros((experts, tokens), F32)
            share = jnp.zeros((experts, tokens), F32)
            for k in range(TOP):
                hit = ids[k:k + 1, :] == names
                member = jnp.where(hit, 1.0, member)
                share = jnp.where(hit, shares[k:k + 1, :], share)
            members.append(member)
            weights.append(share)
    earlier = (
        lax.broadcasted_iota(jnp.int32, (tokens, tokens), 0)
        < lax.broadcasted_iota(jnp.int32, (tokens, tokens), 1)
    )
    member = jnp.concatenate(members, axis=0)
    before = jnp.dot(
        member.astype(BF16), earlier.astype(F32).astype(BF16), preferred_element_type=F32
    )
    place_ref[...] = jnp.where(member > 0.0, before, -1.0).reshape(place_ref.shape)
    if share_ref is not None:
        share_ref[...] = jnp.concatenate(weights, axis=0).reshape(share_ref.shape)


def select_kernel(tiles, names_ref, *refs):
    blocks, metas = refs[:SIDE], refs[SIDE:2 * SIDE]
    outs, place_ref = refs[2 * SIDE:4 * SIDE], refs[4 * SIDE]
    capacity = outs[0].shape[2]
    experts = 2 * SIDE
    step = pl.program_id(0)

    @pl.when(step == 0)
    def _():
        settle(names_ref, metas, place_ref)

    tokens = metas[0].shape[2]
    slot = lax.broadcasted_iota(jnp.int32, (experts, capacity, tokens), 1).astype(F32)
    for i, j in [(i, j) for i in range(BATCH) for j in range(SIDE)]:
        block = blocks[j]
        place = place_ref[step * BATCH + i]
        pick = place[j * experts:(j + 1) * experts][:, None, :] == slot
        pick = pick.astype(F32).reshape(experts * capacity, tokens).astype(BF16)
        features = jnp.concatenate(
            [block[i, n * LANES:(n + 1) * LANES, :] for n in range(tiles)], axis=1
        )
        out = jnp.dot(pick, features, preferred_element_type=F32).astype(BF16)
        for p in range(SIDE):
            for e in range(2):
                row = (2 * p + e) * capacity
                outs[e * SIDE + p][i, j] = out[row:row + capacity, :]


def select(names, blocks, tiles, capacity):
    rows, width = blocks[0].shape[1], tiles * LANES
    at = width // META
    return pl.pallas_call(
        functools.partial(select_kernel, tiles),
        grid_spec=pltpu.PrefetchScalarGridSpec(
            num_scalar_prefetch=1,
            grid=(SIDE // BATCH,),
            in_specs=[pl.BlockSpec((BATCH, rows, LANES), lambda i, s: (i, 0, 0))] * SIDE
            + [pl.BlockSpec((SIDE, META, LANES), lambda i, s: (0, at, 0))] * SIDE,
            out_specs=[
                pl.BlockSpec((BATCH, SIDE, capacity, width), lambda i, s: (i, 0, 0, 0))
            ] * (2 * SIDE),
            scratch_shapes=[pltpu.VMEM((SIDE, 2 * SIDE * SIDE, LANES), F32)],
        ),
        out_shape=[jax.ShapeDtypeStruct((SIDE, SIDE, capacity, width), BF16)] * (2 * SIDE),
    )(names, *blocks, *blocks)


def combine_kernel(width, names_ref, *refs):
    metas, backs = refs[:SIDE], refs[SIDE:3 * SIDE]
    outs, place_ref, share_ref = refs[3 * SIDE:4 * SIDE], refs[4 * SIDE], refs[4 * SIDE + 1]
    capacity, full = backs[0].shape[2:]
    experts = 2 * SIDE
    slots = experts * capacity
    step = pl.program_id(0)

    @pl.when(step == 0)
    def _():
        settle(names_ref, metas, place_ref, share_ref)

    tokens = metas[0].shape[2]
    owner = lax.broadcasted_iota(jnp.int32, (experts, slots), 1) // capacity
    spread = (owner == lax.broadcasted_iota(jnp.int32, (experts, slots), 0))
    spread = spread.astype(F32).astype(BF16)
    slot = (lax.broadcasted_iota(jnp.int32, (tokens, slots), 1) % capacity).astype(F32)
    across = (((0,), (0,)), ((), ()))
    for i, j in [(i, j) for i in range(BATCH) for j in range(SIDE)]:
        here = slice(j * experts, (j + 1) * experts)
        place = place_ref[step * BATCH + i].astype(BF16)
        share = share_ref[step * BATCH + i].astype(BF16)
        taken = lax.dot_general(place[here], spread, across, preferred_element_type=F32)
        weight = lax.dot_general(share[here], spread, across, preferred_element_type=F32)
        pick = taken == slot
        weighted = jnp.where(pick, weight, 0.0).astype(BF16)
        back = jnp.concatenate(
            [backs[e * SIDE + p][i, j] for p in range(SIDE) for e in range(2)], axis=0
        )
        out = jnp.dot(weighted, back[:, :width], preferred_element_type=F32)
        outs[j][i, :, 0:width] = out.astype(BF16)
        if full > width:
            found = jnp.dot(
                pick.astype(F32).astype(BF16), back[:, width:], preferred_element_type=F32
            )
            outs[j][i, :, width:full] = found.astype(BF16)


def combine_slots(names, blocks, backs, tiles):
    capacity, full = backs[0].shape[2:]
    tokens = LANES
    at = tiles * LANES // META
    return pl.pallas_call(
        functools.partial(combine_kernel, tiles * LANES),
        grid_spec=pltpu.PrefetchScalarGridSpec(
            num_scalar_prefetch=1,
            grid=(SIDE // BATCH,),
            in_specs=[pl.BlockSpec((SIDE, META, LANES), lambda i, s: (0, at, 0))] * SIDE
            + [pl.BlockSpec((BATCH, SIDE, capacity, full), lambda i, s: (i, 0, 0, 0))] * (2 * SIDE),
            out_specs=[pl.BlockSpec((BATCH, tokens, full), lambda i, s: (i, 0, 0))] * SIDE,
            scratch_shapes=[pltpu.VMEM((SIDE, 2 * SIDE * SIDE, LANES), F32)] * 2,
        ),
        out_shape=[jax.ShapeDtypeStruct((SIDE, tokens, full), BF16)] * SIDE,
    )(names, *blocks, *backs)


def hidden_kernel(
    expert, table_ref, core_ref, *refs,
):
    wide, narrow = refs[:SIDE], refs[SIDE:2 * SIDE]
    down_mine, down_sent, out_ref, wide_v, narrow_v, down_v, sems = refs[2 * SIDE:]
    step = pl.program_id(0)
    groups, capacity, _ = wide_v.shape
    half = down_v.shape[0] // 2
    width = down_v.shape[1]
    batch = out_ref.shape[0] // capacity
    column = pl.multiple_of(core_ref[0] * width, LANES)
    copies = []
    per = groups // SIDE
    for p in range(SIDE):
        copies.append((wide[p], wide_v.at[p * per:(p + 1) * per]))
        copies.append((narrow[p], narrow_v.at[p * per:(p + 1) * per]))
    copies.append((down_mine.at[expert, :, pl.ds(column, width)], down_v.at[0:half]))
    copies.append((down_sent.at[expert, :, pl.ds(column, width)], down_v.at[half:2 * half]))
    copies = [
        pltpu.make_async_copy(a, b, sems.at[i]) for i, (a, b) in enumerate(copies)
    ]

    @pl.when(step == 0)
    def _():
        for copy in copies:
            copy.start()
        for copy in copies:
            copy.wait()

    first = step * batch
    rows = []
    for j in range(batch):
        rows.append(jnp.concatenate(
            [wide_v[table_ref[first + j]], narrow_v[table_ref[groups + first + j]]], axis=1
        ))
    out = lax.dot_general(
        jnp.concatenate(rows, axis=0), down_v[...], NT, preferred_element_type=F32
    )
    out_ref[...] = out.astype(BF16)


def hidden_step(expert, table, core, wide, narrow, down_mine, down_sent):
    groups = SIDE ** 3
    capacity, wide_width = wide[0].shape[1:]
    narrow_width = narrow[0].shape[2]
    width = wide_width + narrow_width
    hidden = 2 * down_mine.shape[1]
    batch = 256 // capacity
    hbm = pl.BlockSpec(memory_space=pl.ANY)
    return pl.pallas_call(
        functools.partial(hidden_kernel, expert),
        grid_spec=pltpu.PrefetchScalarGridSpec(
            num_scalar_prefetch=2,
            grid=(groups // batch,),
            in_specs=[hbm] * (2 * SIDE + 2),
            out_specs=pl.BlockSpec((batch * capacity, hidden), lambda i, *s: (i, 0)),
            scratch_shapes=[
                pltpu.VMEM((groups, capacity, wide_width), BF16),
                pltpu.VMEM((groups, capacity, narrow_width), BF16),
                pltpu.VMEM((hidden, width), BF16),
                pltpu.SemaphoreType.DMA((2 * SIDE + 2,)),
            ],
        ),
        out_shape=jax.ShapeDtypeStruct((groups * capacity, hidden), BF16),
        compiler_params=pltpu.CompilerParams(vmem_limit_bytes=56 * 1024 * 1024),
    )(table, core, *wide, *narrow, down_mine, down_sent)


def ready_kernel(gate_own, gate_other, up_own, up_other, *outs):
    for i, (gate_ref, up_ref) in enumerate(((gate_own, up_own), (gate_other, up_other))):
        gate = gate_ref[...].astype(F32)
        up = up_ref[...].astype(F32)
        s = jax.nn.sigmoid(gate)
        act = gate * s
        outs[3 * i][...] = act.astype(BF16)
        outs[3 * i + 1][...] = (up * (s * (1.0 + gate * (1.0 - s)))).astype(BF16)
        outs[3 * i + 2][...] = (act * up).astype(BF16)


def ready(saved):
    experts, rows, half = saved[0].shape
    batch = 256
    spec = pl.BlockSpec((1, batch, half), lambda e, i: (e, i, 0))
    return pl.pallas_call(
        ready_kernel,
        grid=(experts, rows // batch),
        in_specs=[spec] * 4,
        out_specs=[spec] * 6,
        out_shape=[jax.ShapeDtypeStruct(saved[0].shape, BF16)] * 6,
        name="ready",
    )(*saved)


def slot_kernel(
    expert, table_ref, core_ref, mine, sent,
    act_own, mix_own, both_own, act_other, mix_other, both_other,
    gatew_mine, gatew_sent, upw_mine, upw_sent, *refs,
):
    wide_out, narrow_out = refs[:SIDE], refs[SIDE:2 * SIDE]
    wide_v, narrow_v, mix_v, sems, out_sems = refs[2 * SIDE:]
    step = pl.program_id(0)
    groups, capacity, wide_full = wide_v.shape
    narrow_width = narrow_v.shape[2]
    width, quad = mix_v.shape
    wide_width = width - narrow_width
    half = quad // 4
    row = pl.multiple_of(core_ref[0] * width, LANES)
    copies = []
    for n, (a, b) in enumerate(((gatew_mine, gatew_sent), (upw_mine, upw_sent))):
        left = 2 * n * half
        copies.append(pltpu.make_async_copy(
            a.at[expert, pl.ds(row, width)], mix_v.at[:, left:left + half], sems.at[2 * n]))
        copies.append(pltpu.make_async_copy(
            b.at[expert, pl.ds(row, width)], mix_v.at[:, left + half:left + 2 * half], sems.at[2 * n + 1]))

    @pl.when(step == 0)
    def _():
        for copy in copies:
            copy.start()

    rows = mine.shape[0]
    batch = rows // capacity
    parts = []
    totals = []
    held = ((act_own, mix_own, both_own), (act_other, mix_other, both_other))
    for i, (act_ref, mix_ref, both_ref) in enumerate(held):
        a, b = i * half, (1 - i) * half
        g = mine[:, a:a + half].astype(F32) + sent[:, b:b + half].astype(F32)
        product = g * both_ref[0].astype(F32)
        parts.append((g * mix_ref[0].astype(F32)).astype(BF16))
        parts.append((g * act_ref[0].astype(F32)).astype(BF16))
        total = product[:, 0:LANES]
        for j in range(1, half // LANES):
            total = total + product[:, j * LANES:(j + 1) * LANES]
        totals.append(total)
    found = jnp.sum(totals[0] + totals[1], axis=1, keepdims=True)
    lane = lax.broadcasted_iota(jnp.int32, (rows, LANES), 1)
    found = jnp.where(lane == core_ref[1] + expert, found, 0.0).astype(BF16)

    @pl.when(step == 0)
    def _():
        for copy in copies:
            copy.wait()

    out = lax.dot_general(
        jnp.concatenate([parts[0], parts[2], parts[1], parts[3]], axis=1),
        mix_v[...], NT, preferred_element_type=F32,
    ).astype(BF16)
    for j in range(batch):
        here = slice(j * capacity, (j + 1) * capacity)
        at_wide = table_ref[step * batch + j]
        at_narrow = table_ref[groups + step * batch + j]
        wide_v[at_wide, :, 0:wide_width] = out[here, 0:wide_width]
        wide_v[at_wide, :, wide_width:wide_full] = found[here, :]
        narrow_v[at_narrow] = out[here, wide_width:width]

    @pl.when(step == pl.num_programs(0) - 1)
    def _():
        per = groups // SIDE
        leave = []
        for p in range(SIDE):
            leave.append(pltpu.make_async_copy(
                wide_v.at[p * per:(p + 1) * per], wide_out[p], out_sems.at[2 * p]))
            leave.append(pltpu.make_async_copy(
                narrow_v.at[p * per:(p + 1) * per], narrow_out[p], out_sems.at[2 * p + 1]))
        for copy in leave:
            copy.start()
        for copy in leave:
            copy.wait()


def slot_step(expert, table, core, mine, sent, saved, weights, capacity, wide_width, narrow_width):
    groups = SIDE ** 3
    rows, hidden = mine.shape
    half = hidden // 2
    batch = 256
    per = groups // SIDE
    hbm = pl.BlockSpec(memory_space=pl.ANY)
    block = pl.BlockSpec((batch, hidden), lambda i, *s: (i, 0))
    kept = pl.BlockSpec((1, batch, half), lambda i, *s: (expert, i, 0))
    wide_full = wide_width + LANES
    width = wide_width + narrow_width
    return pl.pallas_call(
        functools.partial(slot_kernel, expert),
        grid_spec=pltpu.PrefetchScalarGridSpec(
            num_scalar_prefetch=2,
            grid=(rows // batch,),
            in_specs=[block, block] + [kept] * 6 + [hbm] * 4,
            out_specs=[hbm] * (2 * SIDE),
            scratch_shapes=[
                pltpu.VMEM((groups, capacity, wide_full), BF16),
                pltpu.VMEM((groups, capacity, narrow_width), BF16),
                pltpu.VMEM((width, 4 * half), BF16),
                pltpu.SemaphoreType.DMA((4,)),
                pltpu.SemaphoreType.DMA((2 * SIDE,)),
            ],
        ),
        out_shape=[jax.ShapeDtypeStruct((per, capacity, wide_full), BF16)] * SIDE
        + [jax.ShapeDtypeStruct((per, capacity, narrow_width), BF16)] * SIDE,
        compiler_params=pltpu.CompilerParams(vmem_limit_bytes=56 * 1024 * 1024),
    )(table, core, mine, sent, *saved, *weights)


def total_of(parts):
    total = parts[0].astype(F32)
    for part in parts[1:]:
        total = total + part.astype(F32)
    return total


def finish_kernel(ids_ref, *refs):
    wide, narrow = refs[:SIDE], refs[SIDE:2 * SIDE]
    tokens_ref, grad_combine_ref = refs[2 * SIDE:]
    tokens = tokens_ref.shape[0]
    wide_width = wide[0].shape[1] - LANES
    total = total_of([ref[...] for ref in wide])
    tokens_ref[:, 0:wide_width] = total[:, 0:wide_width].astype(BF16)
    tokens_ref[:, wide_width:] = total_of([ref[...] for ref in narrow]).astype(BF16)
    found = total[:, wide_width:].T
    names = lax.broadcasted_iota(jnp.int32, (LANES, tokens), 0)
    rows = [
        jnp.sum(jnp.where(ids_ref[k:k + 1, :] == names, found, 0.0), axis=0, keepdims=True)
        for k in range(TOP)
    ]
    grad_combine_ref[...] = jnp.concatenate(rows, axis=0).astype(BF16)


def finish(ids, wide, narrow):
    tokens = wide[0].shape[0]
    width = wide[0].shape[1] - LANES + narrow[0].shape[1]
    return pl.pallas_call(
        finish_kernel,
        out_shape=[
            jax.ShapeDtypeStruct((tokens, width), BF16),
            jax.ShapeDtypeStruct((TOP, tokens), BF16),
        ],
        name="finish",
    )(ids, *wide, *narrow)


def on_device(
    grad_out, combine, expert_ids, saved_gate, saved_up, gate_weight, up_weight, down_weight
):
    groups = lax.axis_size("expert")
    core = lax.axis_index("etp")
    chip = lax.axis_index("expert")
    width = grad_out.shape[1]
    capacity = saved_gate.shape[0] // groups
    ids, shares = expert_ids.T, combine.T
    tiles = (9, width // LANES - 9)
    lanes = (WIDE, NARROW)

    me = jnp.stack(coords(chip))
    order = jnp.stack(coords(jnp.arange(groups, dtype=jnp.int32)))
    apart = (order - me[:, None]) % SIDE
    tables, names = [], []
    for lane in lanes:
        axes = jnp.where(core == 0, jnp.array(lane[0]), jnp.array(lane[1]))
        step = jnp.take(apart, axes, axis=0)
        tables.append(step[2] * SIDE * SIDE + step[0] * SIDE + step[1])
        along = jnp.arange(SIDE, dtype=jnp.int32)[None, :] * (
            jnp.arange(3)[:, None] == axes[2]
        )
        column = joined((me[:, None] + along) % SIDE)
        names.append((column[:, None] * 2 + jnp.arange(2)[None, :]).reshape(-1).astype(jnp.int32))
    table = jnp.concatenate(tables).astype(jnp.int32)
    place = jnp.stack([core, chip * 2]).astype(jnp.int32)

    blocks = prepare(grad_out, ids, shares, tiles)
    stage = []
    for n, lane in enumerate(lanes):
        parts = gathered(blocks[n], lane, 0)
        stage.append(jnp.stack(parts))
    stage = [gathered(b, lane, 1) for b, lane in zip(stage, lanes)]
    arrived = [[], []]
    for n, lane in enumerate(lanes):
        slots = select(names[n], stage[n], tiles[n], capacity)
        for e in range(2):
            got = scattered(slots[e * SIDE:(e + 1) * SIDE], lane, 2)
            arrived[e].append([x.reshape(SIDE * SIDE, capacity, x.shape[-1]) for x in got])

    swap = [(0, 1), (1, 0)]

    def swapped(x):
        return lax.ppermute(x, "etp", swap)

    saved = []
    for x in (saved_gate, saved_up):
        own = x.transpose(1, 0, 2)
        saved += [own, swapped(own)]
    down_sent, gate_sent, up_sent = [swapped(x) for x in (down_weight, gate_weight, up_weight)]
    saved = ready(saved)

    mine, sent = [], []
    for e in range(2):
        mine.append(
            hidden_step(e, table, place, arrived[e][0], arrived[e][1], down_weight, down_sent)
        )
        sent.append(swapped(mine[e]))
    returned = [[], []]
    for e in range(2):
        pieces = slot_step(
            e, table, place, mine[e], sent[e], saved,
            (gate_weight, gate_sent, up_weight, up_sent),
            capacity, tiles[0] * LANES, tiles[1] * LANES,
        )
        for n, lane in enumerate(lanes):
            backs = [
                x.reshape(SIDE, SIDE, capacity, x.shape[-1])
                for x in pieces[n * SIDE:(n + 1) * SIDE]
            ]
            returned[n] += scattered(backs, lane, 2)
    ends = []
    for n, lane in enumerate(lanes):
        backs = returned[n]
        backs = combine_slots(names[n], stage[n], backs, tiles[n])
        backs = scattered(backs, lane, 1)
        total = [total_of([b[i] for b in backs]).astype(BF16) for i in range(SIDE)]
        ends.append(scattered(total, lane, 0))
    grad_tokens, grad_combine = finish(ids, ends[0], ends[1])
    return grad_tokens, grad_combine.T


def solution(mesh):
    in_specs = (
        P("expert", "etp"),
        P("expert", None),
        P("expert", None),
        P(None, "expert", "etp"),
        P(None, "expert", "etp"),
        P("expert", None, "etp"),
        P("expert", None, "etp"),
        P("expert", "etp", None),
    )
    out_specs = (P("expert", "etp"), P("expert", None))

    return jax.shard_map(
        on_device, mesh=mesh, in_specs=in_specs, out_specs=out_specs, check_vma=False
    )
```

```python
import functools

import jax
import jax.numpy as jnp
from jax import lax
from jax.experimental import pallas as pl
from jax.experimental.pallas import tpu as pltpu
from jax.sharding import PartitionSpec as P


BOTH = ("expert", "etp")
SIDE = 4
TOP = 8
LANES = 128
META = 16
BATCH = 2
ROWS = 256
WIDE_OUT = 9
WIDE_BACK = 9
SEND = (2, 1, 3)
F32 = jnp.float32
BF16 = jnp.bfloat16
WIDE = ((0, 1, 2), (1, 2, 0))
NARROW = ((2, 0, 1), (2, 0, 1))
NT = (((1,), (1,)), ((), ()))


def room(mib):
    return pltpu.CompilerParams(vmem_limit_bytes=mib * 1024 * 1024)


def coords(e):
    return [e // (SIDE * SIDE), (e // SIDE) % SIDE, e % SIDE]


def joined(c):
    return (c[0] * SIDE + c[1]) * SIDE + c[2]


def moved(x, lane, stage, distance):
    pairs = []
    for e in range(SIDE ** 3):
        for core in range(2):
            to = coords(e)
            axis = lane[core][stage]
            to[axis] = (to[axis] - distance) % SIDE
            pairs.append((e * 2 + core, joined(to) * 2 + core))
    return lax.ppermute(x, BOTH, pairs)


def gathered(x, lane, stage):
    got = {q: moved(x, lane, stage, q) for q in SEND}
    return [x, got[1], got[2], got[3]]


def scattered(parts, lane, stage):
    got = {q: moved(parts[-q % SIDE], lane, stage, q) for q in SEND}
    return [parts[0], got[1], got[2], got[3]]


def prepare_kernel(tiles, grad_ref, ids_ref, share_ref, *outs):
    first = 0
    for out, count in zip(outs, tiles):
        for i in range(count):
            column = (first + i) * LANES
            out[i * LANES:(i + 1) * LANES, :] = grad_ref[:, column:column + LANES]
        out[count * LANES:count * LANES + TOP, :] = ids_ref[...].astype(F32).astype(BF16)
        out[count * LANES + TOP:count * LANES + META, :] = share_ref[...]
        first += count


def prepare(grad_out, ids, shares, tiles):
    return pl.pallas_call(
        functools.partial(prepare_kernel, tiles),
        out_shape=[jax.ShapeDtypeStruct((n * LANES + META, LANES), BF16) for n in tiles],
        name="prepare",
    )(grad_out, ids, shares)


def settle(names_ref, metas, place_ref, share_ref=None):
    tokens = metas[0].shape[2]
    experts = 2 * SIDE
    at = lax.broadcasted_iota(jnp.int32, (experts, tokens), 0)
    names = jnp.zeros((experts, tokens), jnp.int32)
    for i in range(experts):
        names = jnp.where(at == i, names_ref[i], names)
    names = names.astype(F32)
    members, weights = [], []
    for i in range(SIDE):
        for j in range(SIDE):
            ids = metas[j][i, 0:TOP, :].astype(F32)
            shares = metas[j][i, TOP:META, :].astype(F32)
            member = jnp.zeros((experts, tokens), F32)
            share = jnp.zeros((experts, tokens), F32)
            for k in range(TOP):
                hit = ids[k:k + 1, :] == names
                member = jnp.where(hit, 1.0, member)
                share = jnp.where(hit, shares[k:k + 1, :], share)
            members.append(member)
            weights.append(share)
    earlier = (
        lax.broadcasted_iota(jnp.int32, (tokens, tokens), 0)
        < lax.broadcasted_iota(jnp.int32, (tokens, tokens), 1)
    )
    member = jnp.concatenate(members, axis=0)
    before = jnp.dot(
        member.astype(BF16), earlier.astype(F32).astype(BF16), preferred_element_type=F32
    )
    place_ref[...] = jnp.where(member > 0.0, before, -1.0).reshape(place_ref.shape)
    if share_ref is not None:
        share_ref[...] = jnp.concatenate(weights, axis=0).reshape(share_ref.shape)


def select_kernel(tiles, names_ref, *refs):
    blocks, metas = refs[:SIDE], refs[SIDE:2 * SIDE]
    outs, place_ref = refs[2 * SIDE:4 * SIDE], refs[4 * SIDE]
    capacity = outs[0].shape[2]
    experts = 2 * SIDE
    step = pl.program_id(0)

    @pl.when(step == 0)
    def _():
        settle(names_ref, metas, place_ref)

    tokens = metas[0].shape[2]
    slot = lax.broadcasted_iota(jnp.int32, (experts, capacity, tokens), 1).astype(F32)
    for i, j in [(i, j) for i in range(BATCH) for j in range(SIDE)]:
        block = blocks[j]
        place = place_ref[step * BATCH + i]
        pick = place[j * experts:(j + 1) * experts][:, None, :] == slot
        pick = pick.astype(F32).reshape(experts * capacity, tokens).astype(BF16)
        features = jnp.concatenate(
            [block[i, n * LANES:(n + 1) * LANES, :] for n in range(tiles)], axis=1
        )
        out = jnp.dot(pick, features, preferred_element_type=F32).astype(BF16)
        for p in range(SIDE):
            for e in range(2):
                row = (2 * p + e) * capacity
                outs[e * SIDE + p][i, j] = out[row:row + capacity, :]


def select(names, blocks, tiles, capacity):
    rows, width = blocks[0].shape[1], tiles * LANES
    at = width // META
    return pl.pallas_call(
        functools.partial(select_kernel, tiles),
        grid_spec=pltpu.PrefetchScalarGridSpec(
            num_scalar_prefetch=1,
            grid=(SIDE // BATCH,),
            in_specs=[pl.BlockSpec((BATCH, rows, LANES), lambda i, s: (i, 0, 0))] * SIDE
            + [pl.BlockSpec((SIDE, META, LANES), lambda i, s: (0, at, 0))] * SIDE,
            out_specs=[
                pl.BlockSpec((BATCH, SIDE, capacity, width), lambda i, s: (i, 0, 0, 0))
            ] * (2 * SIDE),
            scratch_shapes=[pltpu.VMEM((SIDE, 2 * SIDE * SIDE, LANES), F32)],
        ),
        out_shape=[jax.ShapeDtypeStruct((SIDE, SIDE, capacity, width), BF16)] * (2 * SIDE),
        compiler_params=room(24),
    )(names, *blocks, *blocks)


def lots_kernel(names_ref, *refs):
    metas, (weighted_ref, pick_ref) = refs[:SIDE], refs[SIDE:SIDE + 2]
    place_ref, share_ref = refs[SIDE + 2:]
    settle(names_ref, metas, place_ref, share_ref)
    experts = 2 * SIDE
    tokens, slots = weighted_ref.shape[2:]
    capacity = slots // experts
    owner = lax.broadcasted_iota(jnp.int32, (experts, slots), 1) // capacity
    spread = (owner == lax.broadcasted_iota(jnp.int32, (experts, slots), 0))
    spread = spread.astype(F32).astype(BF16)
    slot = (lax.broadcasted_iota(jnp.int32, (tokens, slots), 1) % capacity).astype(F32)
    across = (((0,), (0,)), ((), ()))
    for i, j in [(i, j) for i in range(SIDE) for j in range(SIDE)]:
        here = slice(j * experts, (j + 1) * experts)
        place = place_ref[i, here].astype(BF16)
        share = share_ref[i, here].astype(BF16)
        taken = lax.dot_general(place, spread, across, preferred_element_type=F32)
        weight = lax.dot_general(share, spread, across, preferred_element_type=F32)
        pick = taken == slot
        weighted_ref[i, j] = jnp.where(pick, weight, 0.0).astype(BF16)
        pick_ref[i, j] = pick.astype(F32).astype(BF16)


def lots(names, blocks, tiles, capacity):
    at = tiles * LANES // META
    slots = 2 * SIDE * capacity
    return pl.pallas_call(
        lots_kernel,
        grid_spec=pltpu.PrefetchScalarGridSpec(
            num_scalar_prefetch=1,
            grid=(1,),
            in_specs=[pl.BlockSpec((SIDE, META, LANES), lambda i, s: (0, at, 0))] * SIDE,
            out_specs=[pl.BlockSpec((SIDE, SIDE, LANES, slots), lambda i, s: (0, 0, 0, 0))] * 2,
            scratch_shapes=[pltpu.VMEM((SIDE, 2 * SIDE * SIDE, LANES), F32)] * 2,
        ),
        out_shape=[jax.ShapeDtypeStruct((SIDE, SIDE, LANES, slots), BF16)] * 2,
        compiler_params=room(12),
    )(names, *blocks)


def combine_kernel(width, weighted_ref, pick_ref, *refs):
    backs, outs = refs[:2 * SIDE], refs[2 * SIDE:]
    full = backs[0].shape[3]
    for i, j in [(i, j) for i in range(BATCH) for j in range(SIDE)]:
        back = jnp.concatenate(
            [backs[e * SIDE + p][i, j] for p in range(SIDE) for e in range(2)], axis=0
        )
        out = jnp.dot(weighted_ref[i, j], back[:, :width], preferred_element_type=F32)
        outs[j][i, :, 0:width] = out.astype(BF16)
        if full > width:
            found = jnp.dot(pick_ref[i, j], back[:, width:], preferred_element_type=F32)
            outs[j][i, :, width:full] = found.astype(BF16)


def combine_slots(picks, backs, tiles):
    capacity, full = backs[0].shape[2:]
    slots = picks[0].shape[3]
    tokens = LANES
    return pl.pallas_call(
        functools.partial(combine_kernel, tiles * LANES),
        grid=(SIDE // BATCH,),
        in_specs=[pl.BlockSpec((BATCH, SIDE, tokens, slots), lambda i: (i, 0, 0, 0))] * 2
        + [pl.BlockSpec((BATCH, SIDE, capacity, full), lambda i: (i, 0, 0, 0))] * (2 * SIDE),
        out_specs=[pl.BlockSpec((BATCH, tokens, full), lambda i: (i, 0, 0))] * SIDE,
        out_shape=[jax.ShapeDtypeStruct((SIDE, tokens, full), BF16)] * SIDE,
        compiler_params=room(24),
    )(*picks, *backs)


def hidden_kernel(
    expert, table_ref, core_ref, *refs,
):
    wide, narrow = refs[:SIDE], refs[SIDE:2 * SIDE]
    down_mine, down_sent, out_ref, wide_v, narrow_v, down_v, sems = refs[2 * SIDE:]
    step = pl.program_id(0)
    groups, capacity, _ = wide_v.shape
    half = down_v.shape[0] // 2
    width = down_v.shape[1]
    batch = out_ref.shape[0] // capacity
    column = pl.multiple_of(core_ref[0] * width, LANES)
    copies = []
    per = groups // SIDE
    for p in range(SIDE):
        copies.append((wide[p], wide_v.at[p * per:(p + 1) * per]))
        copies.append((narrow[p], narrow_v.at[p * per:(p + 1) * per]))
    copies.append((down_mine.at[expert, :, pl.ds(column, width)], down_v.at[0:half]))
    copies.append((down_sent.at[expert, :, pl.ds(column, width)], down_v.at[half:2 * half]))
    copies = [
        pltpu.make_async_copy(a, b, sems.at[i]) for i, (a, b) in enumerate(copies)
    ]

    @pl.when(step == 0)
    def _():
        for copy in copies:
            copy.start()
        for copy in copies:
            copy.wait()

    first = step * batch
    rows = []
    for j in range(batch):
        rows.append(jnp.concatenate(
            [wide_v[table_ref[first + j]], narrow_v[table_ref[groups + first + j]]], axis=1
        ))
    out = lax.dot_general(
        jnp.concatenate(rows, axis=0), down_v[...], NT, preferred_element_type=F32
    )
    out_ref[...] = out.astype(BF16)


def hidden_step(expert, table, core, wide, narrow, down_mine, down_sent):
    groups = SIDE ** 3
    capacity, wide_width = wide[0].shape[1:]
    narrow_width = narrow[0].shape[2]
    width = wide_width + narrow_width
    hidden = 2 * down_mine.shape[1]
    batch = ROWS // capacity
    hbm = pl.BlockSpec(memory_space=pl.ANY)
    return pl.pallas_call(
        functools.partial(hidden_kernel, expert),
        grid_spec=pltpu.PrefetchScalarGridSpec(
            num_scalar_prefetch=2,
            grid=(groups // batch,),
            in_specs=[hbm] * (2 * SIDE + 2),
            out_specs=pl.BlockSpec((batch * capacity, hidden), lambda i, *s: (i, 0)),
            scratch_shapes=[
                pltpu.VMEM((groups, capacity, wide_width), BF16),
                pltpu.VMEM((groups, capacity, narrow_width), BF16),
                pltpu.VMEM((hidden, width), BF16),
                pltpu.SemaphoreType.DMA((2 * SIDE + 2,)),
            ],
        ),
        out_shape=jax.ShapeDtypeStruct((groups * capacity, hidden), BF16),
        compiler_params=room(20),
    )(table, core, *wide, *narrow, down_mine, down_sent)


def ready_kernel(gate_own, gate_other, up_own, up_other, *outs):
    for i, (gate_ref, up_ref) in enumerate(((gate_own, up_own), (gate_other, up_other))):
        gate = gate_ref[...].astype(F32)
        up = up_ref[...].astype(F32)
        s = jax.nn.sigmoid(gate)
        act = gate * s
        outs[2 * i][...] = act.astype(BF16)
        outs[2 * i + 1][...] = (up * (s * (1.0 + gate * (1.0 - s)))).astype(BF16)


def ready(saved):
    experts, rows, half = saved[0].shape
    batch = 256
    spec = pl.BlockSpec((1, batch, half), lambda e, i: (e, i, 0))
    return pl.pallas_call(
        ready_kernel,
        grid=(experts, rows // batch),
        in_specs=[spec] * 4,
        out_specs=[spec] * 4,
        out_shape=[jax.ShapeDtypeStruct(saved[0].shape, BF16)] * 4,
        compiler_params=room(24),
        name="ready",
    )(*saved)


def slot_kernel(
    expert, table_ref, core_ref, mine, sent,
    act_own, mix_own, up_own, act_other, mix_other, up_other,
    gatew_mine, gatew_sent, upw_mine, upw_sent, *refs,
):
    wide_out, narrow_out = refs[:SIDE], refs[SIDE:2 * SIDE]
    wide_v, narrow_v, mix_v, sems, out_sems = refs[2 * SIDE:]
    step = pl.program_id(0)
    groups, capacity, wide_full = wide_v.shape
    narrow_width = narrow_v.shape[2]
    width, quad = mix_v.shape
    wide_width = width - narrow_width
    half = quad // 4
    row = pl.multiple_of(core_ref[0] * width, LANES)
    copies = []
    for n, (a, b) in enumerate(((gatew_mine, gatew_sent), (upw_mine, upw_sent))):
        left = 2 * n * half
        copies.append(pltpu.make_async_copy(
            a.at[expert, pl.ds(row, width)], mix_v.at[:, left:left + half], sems.at[2 * n]))
        copies.append(pltpu.make_async_copy(
            b.at[expert, pl.ds(row, width)], mix_v.at[:, left + half:left + 2 * half], sems.at[2 * n + 1]))

    @pl.when(step == 0)
    def _():
        for copy in copies:
            copy.start()

    rows = mine.shape[0]
    batch = rows // capacity
    parts = []
    totals = []
    held = ((act_own, mix_own, up_own), (act_other, mix_other, up_other))
    for i, (act_ref, mix_ref, up_ref) in enumerate(held):
        a, b = i * half, (1 - i) * half
        g = mine[:, a:a + half].astype(F32) + sent[:, b:b + half].astype(F32)
        g_act = g * act_ref[0].astype(F32)
        product = g_act * up_ref[0].astype(F32)
        parts.append((g * mix_ref[0].astype(F32)).astype(BF16))
        parts.append(g_act.astype(BF16))
        total = product[:, 0:LANES]
        for j in range(1, half // LANES):
            total = total + product[:, j * LANES:(j + 1) * LANES]
        totals.append(total)
    found = jnp.sum(totals[0] + totals[1], axis=1, keepdims=True)
    lane = lax.broadcasted_iota(jnp.int32, (rows, LANES), 1)
    found = jnp.where(lane == core_ref[1] + expert, found, 0.0).astype(BF16)

    @pl.when(step == 0)
    def _():
        for copy in copies:
            copy.wait()

    out = lax.dot_general(
        jnp.concatenate([parts[0], parts[2], parts[1], parts[3]], axis=1),
        mix_v[...], NT, preferred_element_type=F32,
    ).astype(BF16)
    for j in range(batch):
        here = slice(j * capacity, (j + 1) * capacity)
        at_wide = table_ref[step * batch + j]
        at_narrow = table_ref[groups + step * batch + j]
        wide_v[at_wide, :, 0:wide_width] = out[here, 0:wide_width]
        wide_v[at_wide, :, wide_width:wide_full] = found[here, :]
        narrow_v[at_narrow] = out[here, wide_width:width]

    @pl.when(step == pl.num_programs(0) - 1)
    def _():
        per = groups // SIDE
        leave = []
        for p in range(SIDE):
            leave.append(pltpu.make_async_copy(
                wide_v.at[p * per:(p + 1) * per], wide_out[p], out_sems.at[2 * p]))
            leave.append(pltpu.make_async_copy(
                narrow_v.at[p * per:(p + 1) * per], narrow_out[p], out_sems.at[2 * p + 1]))
        for copy in leave:
            copy.start()
        for copy in leave:
            copy.wait()


def slot_step(expert, table, core, mine, sent, saved, weights, capacity, wide_width, narrow_width):
    groups = SIDE ** 3
    rows, hidden = mine.shape
    half = hidden // 2
    batch = ROWS
    per = groups // SIDE
    hbm = pl.BlockSpec(memory_space=pl.ANY)
    block = pl.BlockSpec((batch, hidden), lambda i, *s: (i, 0))
    kept = pl.BlockSpec((1, batch, half), lambda i, *s: (expert, i, 0))
    wide_full = wide_width + LANES
    width = wide_width + narrow_width
    return pl.pallas_call(
        functools.partial(slot_kernel, expert),
        grid_spec=pltpu.PrefetchScalarGridSpec(
            num_scalar_prefetch=2,
            grid=(rows // batch,),
            in_specs=[block, block] + [kept] * 6 + [hbm] * 4,
            out_specs=[hbm] * (2 * SIDE),
            scratch_shapes=[
                pltpu.VMEM((groups, capacity, wide_full), BF16),
                pltpu.VMEM((groups, capacity, narrow_width), BF16),
                pltpu.VMEM((width, 4 * half), BF16),
                pltpu.SemaphoreType.DMA((4,)),
                pltpu.SemaphoreType.DMA((2 * SIDE,)),
            ],
        ),
        out_shape=[jax.ShapeDtypeStruct((per, capacity, wide_full), BF16)] * SIDE
        + [jax.ShapeDtypeStruct((per, capacity, narrow_width), BF16)] * SIDE,
        compiler_params=room(30),
    )(table, core, mine, sent, *saved, *weights)


def total_of(parts):
    total = parts[0].astype(F32)
    for part in parts[1:]:
        total = total + part.astype(F32)
    return total


def finish_kernel(ids_ref, *refs):
    wide, narrow = refs[:SIDE], refs[SIDE:2 * SIDE]
    tokens_ref, grad_combine_ref = refs[2 * SIDE:]
    tokens = tokens_ref.shape[0]
    wide_width = wide[0].shape[1] - LANES
    total = total_of([ref[...] for ref in wide])
    tokens_ref[:, 0:wide_width] = total[:, 0:wide_width].astype(BF16)
    tokens_ref[:, wide_width:] = total_of([ref[...] for ref in narrow]).astype(BF16)
    found = total[:, wide_width:].T
    names = lax.broadcasted_iota(jnp.int32, (LANES, tokens), 0)
    rows = [
        jnp.sum(jnp.where(ids_ref[k:k + 1, :] == names, found, 0.0), axis=0, keepdims=True)
        for k in range(TOP)
    ]
    grad_combine_ref[...] = jnp.concatenate(rows, axis=0).astype(BF16)


def finish(ids, wide, narrow):
    tokens = wide[0].shape[0]
    width = wide[0].shape[1] - LANES + narrow[0].shape[1]
    return pl.pallas_call(
        finish_kernel,
        out_shape=[
            jax.ShapeDtypeStruct((tokens, width), BF16),
            jax.ShapeDtypeStruct((TOP, tokens), BF16),
        ],
        compiler_params=room(12),
        name="finish",
    )(ids, *wide, *narrow)


def on_device(
    grad_out, combine, expert_ids, saved_gate, saved_up, gate_weight, up_weight, down_weight
):
    groups = lax.axis_size("expert")
    core = lax.axis_index("etp")
    chip = lax.axis_index("expert")
    width = grad_out.shape[1]
    capacity = saved_gate.shape[0] // groups
    ids, shares = expert_ids.T, combine.T
    tiles = (WIDE_OUT, width // LANES - WIDE_OUT)
    tiles_back = (WIDE_BACK, width // LANES - WIDE_BACK)
    lanes = (WIDE, NARROW)

    me = jnp.stack(coords(chip))
    order = jnp.stack(coords(jnp.arange(groups, dtype=jnp.int32)))
    apart = (order - me[:, None]) % SIDE
    tables, names = [], []
    for lane in lanes:
        axes = jnp.where(core == 0, jnp.array(lane[0]), jnp.array(lane[1]))
        step = jnp.take(apart, axes, axis=0)
        tables.append(step[2] * SIDE * SIDE + step[0] * SIDE + step[1])
        along = jnp.arange(SIDE, dtype=jnp.int32)[None, :] * (
            jnp.arange(3)[:, None] == axes[2]
        )
        column = joined((me[:, None] + along) % SIDE)
        names.append((column[:, None] * 2 + jnp.arange(2)[None, :]).reshape(-1).astype(jnp.int32))
    table = jnp.concatenate(tables).astype(jnp.int32)
    place = jnp.stack([core, chip * 2]).astype(jnp.int32)

    blocks = prepare(grad_out, ids, shares, tiles)
    stage = []
    for n, lane in enumerate(lanes):
        parts = gathered(blocks[n], lane, 0)
        stage.append(jnp.stack(parts))
    stage = [gathered(b, lane, 1) for b, lane in zip(stage, lanes)]
    arrived = [[], []]
    for n, lane in enumerate(lanes):
        slots = select(names[n], stage[n], tiles[n], capacity)
        for e in range(2):
            got = scattered(slots[e * SIDE:(e + 1) * SIDE], lane, 2)
            arrived[e].append([x.reshape(SIDE * SIDE, capacity, x.shape[-1]) for x in got])

    swap = [(0, 1), (1, 0)]

    def swapped(x):
        return lax.ppermute(x, "etp", swap)

    saved = []
    for x in (saved_gate, saved_up):
        own = x.transpose(1, 0, 2)
        saved += [own, swapped(own)]
    down_sent, gate_sent, up_sent = [swapped(x) for x in (down_weight, gate_weight, up_weight)]
    factors = ready(saved)
    saved = (factors[0], factors[1], saved[2], factors[2], factors[3], saved[3])

    mine, sent = [], []
    for e in range(2):
        mine.append(
            hidden_step(e, table, place, arrived[e][0], arrived[e][1], down_weight, down_sent)
        )
        sent.append(swapped(mine[e]))
    returned = [[], []]
    for e in range(2):
        pieces = slot_step(
            e, table, place, mine[e], sent[e], saved,
            (gate_weight, gate_sent, up_weight, up_sent),
            capacity, tiles_back[0] * LANES, tiles_back[1] * LANES,
        )
        for n, lane in enumerate(lanes):
            backs = [
                x.reshape(SIDE, SIDE, capacity, x.shape[-1])
                for x in pieces[n * SIDE:(n + 1) * SIDE]
            ]
            returned[n] += scattered(backs, lane, 2)
    picks = [lots(names[n], stage[n], tiles[n], capacity) for n in range(len(lanes))]
    ends = []
    for n, lane in enumerate(lanes):
        backs = returned[n]
        backs = combine_slots(picks[n], backs, tiles_back[n])
        backs = scattered(backs, lane, 1)
        total = [total_of([b[i] for b in backs]).astype(BF16) for i in range(SIDE)]
        ends.append(scattered(total, lane, 0))
    grad_tokens, grad_combine = finish(ids, ends[0], ends[1])
    return grad_tokens, grad_combine.T


def solution(mesh):
    in_specs = (
        P("expert", "etp"),
        P("expert", None),
        P("expert", None),
        P(None, "expert", "etp"),
        P(None, "expert", "etp"),
        P("expert", None, "etp"),
        P("expert", None, "etp"),
        P("expert", "etp", None),
    )
    out_specs = (P("expert", "etp"), P("expert", None))

    return jax.shard_map(
        on_device, mesh=mesh, in_specs=in_specs, out_specs=out_specs, check_vma=False
    )
```
